32 devices in a mesh: ka: 4 (over y, x), gy: 8 (over z, core).
Axes of the slice: x: 2, y: 2, z: 4, core: 2. Of those that a mesh axis runs over, the one named last changes fastest.
Arguments:
- driving_coefficients: float32 [2, 32768, 2, 192], P(None, 'ka', None, 'gy'), may hold values from -6 to 6
Outputs:
- velocity_coefficients: float32 [2, 32768, 2, 192], P(None, 'ka', None, 'gy')
- spectrum: float32 [2, 192], P(None, 'gy')
The draws below stay inside these ranges and needn't reach their ends.
All inputs are finite; a program needn't handle non-finite values.
Results may differ from the reference program's by a relative error of at most 0.0003.
Values sent between devices are 32-bit elements.
A program may use at most 128 MiB of HBM per device.

```python
import jax
import jax.numpy as jnp
from jax import lax

MODES_Z = 512
NCH = 384
HALF = 192
PAIRS = 32768


def block_levels(rng, extent, pieces, least, top_value):
    factor_of, own = 1.0, jax.random.fold_in(rng, 6)
    for dim, blocks in pieces:
        draws = jnp.exp(jax.random.uniform(jax.random.fold_in(own, dim), (blocks,), jnp.float32, least / len(pieces), top_value / len(pieces)))
        factor_of = factor_of * jnp.repeat(draws, extent[dim] // blocks).reshape([-1 if axis == dim else 1 for axis in range(len(extent))])
    return factor_of


def centred(own_key, dims, deviation, bound, pieces=(), kind=jnp.bfloat16):
    drawn = deviation * jax.random.normal(own_key, dims, jnp.float32)
    if pieces:
        drawn = drawn * block_levels(own_key, dims, pieces, -0.22, 0.18)
    return jnp.clip(drawn, -bound, bound).astype(kind)


def setup_inputs(seed: int = 0) -> dict:
    keys = jax.random.split(jax.random.key(seed), 2)
    return {
        "driving_coefficients": centred(keys[0], (2, PAIRS, 2, HALF), 1.0, 6.0, ((1, 4), (3, 8)), jnp.float32),
    }


viscous_rate = 400.0
wave_x = 1.0
wave_z = 2.0


def helm_shift(pair_ids):
    col_x = pair_ids // MODES_Z
    col_z = pair_ids % MODES_Z
    signed = jnp.where(col_z < MODES_Z // 2, col_z, col_z - MODES_Z)
    wave_kx = wave_x * col_x.astype(jnp.float32)
    wave_kz = wave_z * signed.astype(jnp.float32)
    return wave_kx * wave_kx + wave_kz * wave_kz + viscous_rate


def row_weights(glob_rows):
    parity = jnp.arange(2, dtype=jnp.int32)
    order_int = 2 * glob_rows[None, :] + parity[:, None]
    top_row = jnp.broadcast_to((glob_rows == 0)[None, :], order_int.shape)
    degree = jnp.where(top_row, 4, order_int).astype(jnp.float32)
    lower_w = jnp.where(order_int == 2, 2.0, 1.0) / (4.0 * degree * (degree - 1.0))
    middle_w = jnp.where(order_int <= NCH - 3, 1.0, 0.0) / (2.0 * (degree * degree - 1.0))
    upper_w = jnp.where(order_int + 2 <= NCH - 3, 1.0, 0.0) / (4.0 * degree * (degree + 1.0))
    lower_w = jnp.where(top_row, 0.0, lower_w)
    middle_w = jnp.where(top_row, 0.0, middle_w)
    upper_w = jnp.where(top_row, 0.0, upper_w)
    return top_row, lower_w, middle_w, upper_w


def system(shift_sq, glob_rows, padded):
    top_row, lower_w, middle_w, upper_w = row_weights(glob_rows)
    shift_col = shift_sq[:, None, None]
    lower_band = shift_col * lower_w
    diag_band = jnp.where(top_row, 1.0, -(1.0 + shift_col * middle_w))
    above_diagonal_entries = shift_col * upper_w
    source = -viscous_rate * (lower_w * padded[..., :-2] - middle_w * padded[..., 1:-1] + upper_w * padded[..., 2:])
    single_forcing_vector = jnp.broadcast_to(jnp.where(top_row, 1.0, 0.0), lower_band.shape).astype(source.dtype)
    sources = jnp.concatenate([source, single_forcing_vector[None]], axis=0)
    return lower_band, diag_band, above_diagonal_entries, sources


def eliminate(lower_band, diag_band, above_diagonal_entries, sources, factor_in, offset_in):
    def advance(running, row_stack):
        factor, offset = running
        row_low, row_diag, row_high, row_src = row_stack
        pivot_row = row_diag - row_low * factor
        updated_multiplier = row_high / pivot_row
        offset_new = (row_src - row_low * offset) / pivot_row
        return (updated_multiplier, offset_new), (updated_multiplier, offset_new)

    stacked = (jnp.moveaxis(lower_band, -1, 0), jnp.moveaxis(diag_band, -1, 0),
               jnp.moveaxis(above_diagonal_entries, -1, 0), jnp.moveaxis(sources, -1, 0))
    return lax.scan(advance, (factor_in, offset_in), stacked)[1]


def substitute(factors, starting_positions, start_in):
    def retreat(running, row_pair):
        line_multiplier, row_offset = row_pair
        result = row_offset - line_multiplier * running
        return result, result

    return jnp.moveaxis(lax.scan(retreat, start_in, (factors, starting_positions), reverse=True)[1], 0, -1)


def closing(columns, sum_free, sum_unit):
    wall_coef = -sum_free / sum_unit
    return columns[:2] + wall_coef[..., None] * columns[2][None]


def reference(driving_coefficients):
    pair_ids = jnp.arange(PAIRS, dtype=jnp.int32)
    shift_sq = helm_shift(pair_ids)
    glob_rows = jnp.arange(HALF, dtype=jnp.int32)
    padded = jnp.pad(driving_coefficients, ((0, 0), (0, 0), (0, 0), (1, 1)))
    lower_band, diag_band, above_diagonal_entries, sources = system(shift_sq, glob_rows, padded)
    zeros_p = jnp.zeros((PAIRS, 2), jnp.float32)
    zeros_v = jnp.zeros((3, PAIRS, 2), jnp.float32)
    factors, starting_positions = eliminate(lower_band, diag_band, above_diagonal_entries, sources, zeros_p, zeros_v)
    columns = substitute(factors, starting_positions, zeros_v)
    velocity_coefficients = closing(columns, jnp.sum(columns[:2], axis=-1), jnp.sum(columns[2], axis=-1))
    spectrum = jnp.sum(velocity_coefficients * velocity_coefficients, axis=(0, 1)) / (2.0 * PAIRS)
    return velocity_coefficients, spectrum
```

```python
import functools

import jax
import jax.numpy as jnp
import numpy as np
from jax import lax
from jax.experimental import pallas as pl
from jax.experimental.pallas import tpu as pltpu
from jax.sharding import PartitionSpec as P

MODES_Z = 512
LANES = 128
MESH = pl.DeviceIdType.MESH

viscous_rate = 400.0
wave_x = 1.0
wave_z = 2.0


def weight_table(total_rows):
    nch = 2 * total_rows
    rows = np.arange(total_rows + 1)
    order = 2 * rows[None, :] + np.arange(2)[:, None]
    top = np.broadcast_to((rows == 0)[None, :], order.shape)
    degree = np.where(top, 4, order).astype(np.float64)
    lower = np.where(order == 2, 2.0, 1.0) / (4.0 * degree * (degree - 1.0))
    middle = np.where(order <= nch - 3, 1.0, 0.0) / (2.0 * (degree * degree - 1.0))
    upper = np.where(order + 2 <= nch - 3, 1.0, 0.0) / (4.0 * degree * (degree + 1.0))
    lower, middle, upper = (np.where(top, 0.0, w) for w in (lower, middle, upper))
    cross = upper[:, :-1] * lower[:, 1:]
    return np.stack([lower[:, :-1], middle[:, :-1], upper[:, :-1], cross]).astype(np.float32).reshape(-1)


def shift_of(first_pair, rows):
    shape = (rows, LANES)
    pair = first_pair + lax.broadcasted_iota(jnp.int32, shape, 0) * LANES + lax.broadcasted_iota(jnp.int32, shape, 1)
    col_x = lax.shift_right_logical(pair, MODES_Z.bit_length() - 1)
    col_z = lax.bitwise_and(pair, MODES_Z - 1)
    signed = jnp.where(col_z < MODES_Z // 2, col_z, col_z - MODES_Z)
    kx = wave_x * col_x.astype(jnp.float32)
    kz = wave_z * signed.astype(jnp.float32)
    return kx * kx + kz * kz + viscous_rate


def row_factors(w_ref, total, q, row, local, last, lam, lam2, s_next):
    at = lambda k: w_ref[(2 * k + q) * total + row]
    pivot = 1.0 + lam * at(1)
    if local < last:
        pivot = pivot - lam2 * at(3) * s_next
    s = 1.0 / pivot
    low = lam * at(0)
    if local == 0:
        low = low + jnp.where(row == 0, 1.0, 0.0)
    return s, low * s, lam * at(2)


def reduce_kernel(n, per, rows, tile, group, w_ref, f_hbm, out_ref,
                  f_buf, y_send, y_recv, coef, elim, b_send, b_recv,
                  load_sem, ysend_sem, yrecv_sem, bsend_sem, brecv_sem):
    total = n * rows
    last = rows - 1
    me = lax.axis_index("gy")
    ka = lax.axis_index("ka")
    pairs = n * per * LANES
    span = group * per * tile
    groups = n // group
    first = lax.rem(me // group + 1, groups)

    def load(i):
        g = lax.rem(first + i, groups)
        where = pl.ds(pl.multiple_of(g * span, span), span)
        return pltpu.make_async_copy(f_hbm.at[:, :, :, where, :], f_buf.at[:, :, :, where, :], load_sem.at[i])

    for i in range(groups):
        load(i).start()

    barrier = pltpu.get_barrier_semaphore()

    def greet(k, _):
        pl.semaphore_signal(barrier, inc=1, device_id={"gy": lax.rem(me + k, n)}, device_id_type=MESH)
        return 0

    lax.fori_loop(1, n, greet, 0)

    def y_copy(to, frm):
        return pltpu.make_async_remote_copy(
            src_ref=y_send.at[to], dst_ref=y_recv.at[frm], send_sem=ysend_sem.at[to],
            recv_sem=yrecv_sem.at[frm], device_id={"gy": to}, device_id_type=MESH)

    def b_copy(to, frm):
        return pltpu.make_async_remote_copy(
            src_ref=b_send.at[to], dst_ref=b_recv.at[frm], send_sem=bsend_sem.at[to],
            recv_sem=brecv_sem.at[frm], device_id={"gy": to}, device_id_type=MESH)

    def local_group(i, _):
        g = lax.rem(first + i, groups)
        load(i).wait()
        lam = shift_of(ka * pairs + g * (group * per * LANES), group * per)
        lam2 = lam * lam
        kappa = viscous_rate / lam
        for q in range(2):
            s = None
            e = [None, None]
            yl = [None, None]
            sums = [None, None]
            for j in range(last, -1, -1):
                row = me * rows + j
                s, ls, up = row_factors(w_ref, total, q, row, j, last, lam, lam2, s)
                for p in range(2):
                    f = f_buf[p, q, j // tile, pl.ds(g * span + j % tile, group * per, stride=tile), :]
                    src = kappa * f
                    if j == last:
                        e[p] = s * src
                        yl[p] = e[p]
                        sums[p] = e[p] - src
                    else:
                        e[p] = s * (src + up * e[p])
                        yl[p] = yl[p] + carry * e[p]
                        sums[p] = sums[p] + (theta * e[p] - src)
                if j == last:
                    carry = ls
                    theta = 1.0 + ls
                else:
                    carry = carry * ls
                    theta = 1.0 + ls * theta
            for p in range(2):
                for k, value in enumerate((e[p], yl[p], sums[p])):
                    for m in range(group):
                        y_send[g * group + m, k, p, q] = value[m * per:(m + 1) * per]

        @pl.when(i == 0)
        def _():
            pl.semaphore_wait(barrier, n - 1)

        for m in range(group):
            to = g * group + m

            @pl.when(to != me)
            def _():
                y_copy(to, me).start()
        return 0

    lax.fori_loop(0, groups, local_group, 0)
    y_recv[me] = y_send[me]

    lam = shift_of(ka * pairs + me * (per * LANES), per)
    lam2 = lam * lam
    unroll = 4 if n % 4 == 0 else 1

    def responses(i, _):
        for d in range(unroll):
            block = i * unroll + d
            for q in range(2):
                s = None
                for j in range(last, -1, -1):
                    row = block * rows + j
                    s, ls, up = row_factors(w_ref, total, q, row, j, last, lam, lam2, s)
                    if j == last:
                        e = s * up
                        yl = e
                        sums = e
                        carry = ls
                        tau = ls
                    else:
                        e = s * (up * e)
                        yl = yl + carry * e
                        sums = sums + (1.0 + tau) * e
                        carry = carry * ls
                        tau = ls * (1.0 + tau)
                for k, value in enumerate((ls, e, carry, yl, tau, sums)):
                    coef[block, k, q] = value
        return 0

    lax.fori_loop(0, n // unroll, responses, 0)

    def y_arrived(k, _):
        y_copy(me, lax.rem(me + k, n)).wait_recv()
        return 0

    lax.fori_loop(1, n, y_arrived, 0)

    zero = jnp.zeros((2, per, LANES), jnp.float32)
    for k in range(3):
        elim[n, k] = zero

    def up_sweep(k, state):
        g = n - 1 - k
        f0, f1, phi, s0, s1, psi = state
        a, b, c, d, alpha, beta = (coef[g, m] for m in range(6))
        inv = 1.0 / (1.0 - d * phi)
        lamb = c * inv
        ls = [(y_recv[g, 1, p] + d * fp) * inv for p, fp in ((0, f0), (1, f1))]
        right = [fp + phi * l for fp, l in ((f0, ls[0]), (f1, ls[1]))]
        new_f = [y_recv[g, 0, p] + b * right[p] for p in range(2)]
        new_s = [y_recv[g, 2, p] + beta * right[p] + sp + psi * ls[p] for p, sp in ((0, s0), (1, s1))]
        new_phi = a + b * (phi * lamb)
        new_psi = alpha + beta * (phi * lamb) + psi * lamb
        elim[g, 0] = new_f[0]
        elim[g, 1] = new_f[1]
        elim[g, 2] = new_phi
        elim[g, 3] = ls[0]
        elim[g, 4] = ls[1]
        elim[g, 5] = lamb
        return new_f[0], new_f[1], new_phi, new_s[0], new_s[1], new_psi

    state = lax.fori_loop(0, n, up_sweep, (zero,) * 6)
    wall = 1.0 / state[5]

    def down_sweep(g, left):
        b_send[g, 0, 0] = left[0]
        b_send[g, 0, 1] = left[1]
        new = [elim[g, 3 + p] + elim[g, 5] * left[p] for p in range(2)]
        for p in range(2):
            b_send[g, 1, p] = elim[g + 1, p] + elim[g + 1, 2] * new[p]

        @pl.when(g != me)
        def _():
            b_copy(g, me).start()

        return new[0], new[1]

    lax.fori_loop(0, n, down_sweep, (-state[3] * wall, -state[4] * wall))
    b_recv[me] = b_send[me]
    out_ref[me] = b_recv[me]

    def b_arrived(k, _):
        frm = lax.rem(me + k, n)
        b_copy(me, frm).wait_recv()
        out_ref[frm] = b_recv[frm]
        return 0

    lax.fori_loop(1, n, b_arrived, 0)

    def sent(k, _):
        to = lax.rem(me + k, n)
        y_copy(to, me).wait_send()
        b_copy(to, me).wait_send()
        return 0

    lax.fori_loop(1, n, sent, 0)


def close_kernel(n, per, rows, tile, group, w_ref, f_ref, b_ref, x_ref, sq_ref, e_buf, ls_buf):
    total = n * rows
    last = rows - 1
    me = lax.axis_index("gy")
    ka = lax.axis_index("ka")
    i = pl.program_id(0)
    count = group * per

    @pl.when(i == 0)
    def _():
        sq_ref[...] = jnp.zeros_like(sq_ref)

    lam = shift_of(ka * (n * per * LANES) + i * (count * LANES), count)
    lam2 = lam * lam
    kappa = viscous_rate / lam
    joined = lambda k, p, q: jnp.concatenate([b_ref[m, k, p, q] for m in range(group)], axis=0)
    for q in range(2):
        s = None
        e = [joined(1, p, q) for p in range(2)]
        for j in range(last, -1, -1):
            s, ls, up = row_factors(w_ref, total, q, me * rows + j, j, last, lam, lam2, s)
            ls_buf[q, j] = ls
            for p in range(2):
                f = f_ref[p, q, j // tile, pl.ds(j % tile, count, stride=tile), :]
                e[p] = s * (kappa * f + up * e[p])
                e_buf[q, p, j] = e[p]
        z = [joined(0, p, q) for p in range(2)]
        for j in range(rows):
            square = None
            for p in range(2):
                where = (p, q, j // tile, pl.ds(j % tile, count, stride=tile), slice(None))
                z[p] = e_buf[q, p, j] + ls_buf[q, j] * z[p]
                x = z[p] - kappa * f_ref[where]
                x_ref[where] = x
                square = x * x if p == 0 else square + x * x
            sq_ref[q, j] += sum(square[m * per:(m + 1) * per] for m in range(group))


def spectrum_kernel(nk, rows, scale, sq_ref, out_ref, mine, held, send_sem, recv_sem):
    me = lax.axis_index("ka")
    barrier = pltpu.get_barrier_semaphore()
    for k in range(1, nk):
        pl.semaphore_signal(barrier, inc=1, device_id={"ka": lax.rem(me + k, nk)}, device_id_type=MESH)
    mine[...] = jnp.sum(sq_ref[...], axis=2)
    pl.semaphore_wait(barrier, nk - 1)

    def copy(k):
        return pltpu.make_async_remote_copy(
            src_ref=mine, dst_ref=held.at[k - 1], send_sem=send_sem.at[k - 1], recv_sem=recv_sem.at[k - 1],
            device_id={"ka": lax.rem(me + k, nk)}, device_id_type=MESH)

    for k in range(1, nk):
        copy(k).start()
    added = mine[...]
    for k in range(1, nk):
        copy(k).wait_recv()
        added = added + held[k - 1]
    ones = jnp.ones((8, LANES), jnp.float32)
    for q in range(2):
        sums = lax.dot_general(ones, added[q], (((1,), (1,)), ((), ())), precision=lax.Precision.HIGHEST,
                               preferred_element_type=jnp.float32)
        out_ref[q:q + 1, :] = sums[0:1] * scale
    for k in range(1, nk):
        copy(k).wait_send()


def per_device(n, nk, driving_coefficients):
    _, pairs, _, rows = driving_coefficients.shape
    per = pairs // (LANES * n)
    tile = 8 if rows % 8 == 0 else 1
    cols = pairs // LANES
    group = next((g for g in range(2, n) if n % g == 0 and g * per * tile % 8 == 0), n)
    span = group * per * tile
    f = jnp.transpose(driving_coefficients, (0, 2, 3, 1)).reshape(2, 2, rows // tile, tile, cols, LANES)
    f = jnp.swapaxes(f, 3, 4).reshape(2, 2, rows // tile, cols * tile, LANES)
    table = jnp.asarray(weight_table(n * rows))
    smem = pl.BlockSpec(memory_space=pltpu.SMEM)
    vmem = pl.BlockSpec(memory_space=pltpu.VMEM)
    f32 = jnp.float32
    edges = pl.pallas_call(
        functools.partial(reduce_kernel, n, per, rows, tile, group),
        out_shape=jax.ShapeDtypeStruct((n, 2, 2, 2, per, LANES), f32),
        in_specs=[smem, pl.BlockSpec(memory_space=pl.ANY)],
        out_specs=vmem,
        scratch_shapes=[
            pltpu.VMEM(f.shape, f32),
            pltpu.VMEM((n, 3, 2, 2, per, LANES), f32),
            pltpu.VMEM((n, 3, 2, 2, per, LANES), f32),
            pltpu.VMEM((n, 6, 2, per, LANES), f32),
            pltpu.VMEM((n + 1, 6, 2, per, LANES), f32),
            pltpu.VMEM((n, 2, 2, 2, per, LANES), f32),
            pltpu.VMEM((n, 2, 2, 2, per, LANES), f32),
            pltpu.SemaphoreType.DMA((n // group,)),
            pltpu.SemaphoreType.DMA((n,)),
            pltpu.SemaphoreType.DMA((n,)),
            pltpu.SemaphoreType.DMA((n,)),
            pltpu.SemaphoreType.DMA((n,)),
        ],
        compiler_params=pltpu.CompilerParams(collective_id=0, has_side_effects=True),
        name="reduce_blocks",
    )(table, f)
    block = (2, 2, rows // tile, span, LANES)
    x, squares = pl.pallas_call(
        functools.partial(close_kernel, n, per, rows, tile, group),
        grid=(n // group,),
        out_shape=(jax.ShapeDtypeStruct(f.shape, f32), jax.ShapeDtypeStruct((2, rows, per, LANES), f32)),
        in_specs=[smem, pl.BlockSpec(block, lambda i: (0, 0, 0, i, 0)),
                  pl.BlockSpec((group, 2, 2, 2, per, LANES), lambda i: (i, 0, 0, 0, 0, 0))],
        out_specs=(pl.BlockSpec(block, lambda i: (0, 0, 0, i, 0)),
                   pl.BlockSpec((2, rows, per, LANES), lambda i: (0, 0, 0, 0))),
        scratch_shapes=[pltpu.VMEM((2, 2, rows, group * per, LANES), f32), pltpu.VMEM((2, rows, group * per, LANES), f32)],
        name="close_blocks",
    )(table, f, edges)
    spectrum = pl.pallas_call(
        functools.partial(spectrum_kernel, nk, rows, 1.0 / (2.0 * pairs * nk)),
        out_shape=jax.ShapeDtypeStruct((2, rows), f32),
        in_specs=[vmem],
        out_specs=vmem,
        scratch_shapes=[
            pltpu.VMEM((2, rows, LANES), f32),
            pltpu.VMEM((nk - 1, 2, rows, LANES), f32),
            pltpu.SemaphoreType.DMA((nk - 1,)),
            pltpu.SemaphoreType.DMA((nk - 1,)),
        ],
        compiler_params=pltpu.CompilerParams(collective_id=1, has_side_effects=True),
        name="spectrum_over_ka",
    )(squares)
    x = jnp.swapaxes(x.reshape(2, 2, rows // tile, cols, tile, LANES), 3, 4).reshape(2, 2, rows, pairs)
    return jnp.transpose(x, (0, 3, 1, 2)), spectrum


def solution(mesh):
    n, nk = mesh.shape["gy"], mesh.shape["ka"]
    return jax.shard_map(
        functools.partial(per_device, n, nk), mesh=mesh,
        in_specs=(P(None, "ka", None, "gy"),),
        out_specs=(P(None, "ka", None, "gy"), P(None, "gy")), check_vma=False,
    )
```

```python
import functools

import jax
import jax.numpy as jnp
import numpy as np
from jax import lax
from jax.experimental import pallas as pl
from jax.experimental.pallas import tpu as pltpu
from jax.sharding import PartitionSpec as P

MODES_Z = 512
LANES = 128
MESH = pl.DeviceIdType.MESH

viscous_rate = 400.0
wave_x = 1.0
wave_z = 2.0


def weight_table(total_rows):
    nch = 2 * total_rows
    rows = np.arange(total_rows + 1)
    order = 2 * rows[None, :] + np.arange(2)[:, None]
    top = np.broadcast_to((rows == 0)[None, :], order.shape)
    degree = np.where(top, 4, order).astype(np.float64)
    lower = np.where(order == 2, 2.0, 1.0) / (4.0 * degree * (degree - 1.0))
    middle = np.where(order <= nch - 3, 1.0, 0.0) / (2.0 * (degree * degree - 1.0))
    upper = np.where(order + 2 <= nch - 3, 1.0, 0.0) / (4.0 * degree * (degree + 1.0))
    lower, middle, upper = (np.where(top, 0.0, w) for w in (lower, middle, upper))
    cross = upper[:, :-1] * lower[:, 1:]
    return np.stack([lower[:, :-1], middle[:, :-1], upper[:, :-1], cross]).astype(np.float32).reshape(-1)


def shift_of(first_pair, rows):
    shape = (rows, LANES)
    pair = first_pair + lax.broadcasted_iota(jnp.int32, shape, 0) * LANES + lax.broadcasted_iota(jnp.int32, shape, 1)
    col_x = lax.shift_right_logical(pair, MODES_Z.bit_length() - 1)
    col_z = lax.bitwise_and(pair, MODES_Z - 1)
    signed = jnp.where(col_z < MODES_Z // 2, col_z, col_z - MODES_Z)
    kx = wave_x * col_x.astype(jnp.float32)
    kz = wave_z * signed.astype(jnp.float32)
    return kx * kx + kz * kz + viscous_rate


def row_factors(w_ref, total, q, row, local, last, lam, lam2, s_next):
    at = lambda k: w_ref[(2 * k + q) * total + row]
    pivot = 1.0 + lam * at(1)
    if local < last:
        pivot = pivot - lam2 * at(3) * s_next
    s = 1.0 / pivot
    low = lam * at(0)
    if local == 0:
        low = low + jnp.where(row == 0, 1.0, 0.0)
    return s, low * s, lam * at(2)


def channel_kernel(n, nk, per, rows, tile, group, scale, w_ref, f_hbm, x_hbm, spec_ref,
                   f_buf, x_buf, e_buf, ls_buf, r_buf, sq_buf, y_send, y_recv, coef, elim, b_send, b_recv, mine, held,
                   load_sem, store_sem, ysend_sem, yrecv_sem, bsend_sem, brecv_sem, ssend_sem, srecv_sem):
    total = n * rows
    last = rows - 1
    me = lax.axis_index("gy")
    ka = lax.axis_index("ka")
    pairs = n * per * LANES
    count = group * per
    span = count * tile
    groups = n // group

    def nearest(k, here, size):
        return lax.bitwise_xor(here, k) if size & (size - 1) == 0 else lax.rem(here + k, size)

    def load(i):
        g = nearest(groups - 1 - i, me // group, groups)
        where = pl.ds(pl.multiple_of(g * span, span), span)
        return pltpu.make_async_copy(f_hbm.at[:, :, :, where, :], f_buf.at[:, :, :, where, :], load_sem.at[i])

    def store(i):
        g = nearest(i, me // group, groups)
        where = pl.ds(pl.multiple_of(g * span, span), span)
        return pltpu.make_async_copy(x_buf.at[:, :, :, where, :], x_hbm.at[:, :, :, where, :], store_sem.at[i])

    for i in range(groups):
        load(i).start()

    barrier = pltpu.get_barrier_semaphore()

    def greet(k, _):
        pl.semaphore_signal(barrier, inc=1, device_id={"gy": lax.rem(me + k, n)}, device_id_type=MESH)
        return 0

    lax.fori_loop(1, n, greet, 0)
    for k in range(1, nk):
        pl.semaphore_signal(barrier, inc=1, device_id={"ka": lax.rem(ka + k, nk)}, device_id_type=MESH)

    def y_copy(to, frm):
        return pltpu.make_async_remote_copy(
            src_ref=y_send.at[to], dst_ref=y_recv.at[frm], send_sem=ysend_sem.at[to],
            recv_sem=yrecv_sem.at[frm], device_id={"gy": to}, device_id_type=MESH)

    def b_copy(to, frm):
        return pltpu.make_async_remote_copy(
            src_ref=b_send.at[to], dst_ref=b_recv.at[frm], send_sem=bsend_sem.at[to],
            recv_sem=brecv_sem.at[frm], device_id={"gy": to}, device_id_type=MESH)

    def local_group(i, _):
        g = nearest(groups - 1 - i, me // group, groups)
        load(i).wait()
        part = pl.ds(pl.multiple_of(g * count, count), count)
        lam = shift_of(ka * pairs + g * (count * LANES), count)
        lam2 = lam * lam
        kappa = viscous_rate / lam
        for q in range(2):
            s = None
            e = [None, None]
            yl = [None, None]
            sums = [None, None]
            for j in range(last, -1, -1):
                row = me * rows + j
                s, ls, up = row_factors(w_ref, total, q, row, j, last, lam, lam2, s)
                right = s * up if j == last else (s * up) * right
                ls_buf[q, j, part] = ls
                r_buf[q, j, part] = right
                for p in range(2):
                    f = f_buf[p, q, j // tile, pl.ds(g * span + j % tile, count, stride=tile), :]
                    src = kappa * f
                    if j == last:
                        e[p] = s * src
                        yl[p] = e[p]
                        sums[p] = e[p] - src
                    else:
                        e[p] = s * (src + up * e[p])
                        yl[p] = yl[p] + carry * e[p]
                        sums[p] = sums[p] + (theta * e[p] - src)
                    e_buf[p, q, j, part] = e[p]
                if j == last:
                    carry = ls
                    theta = 1.0 + ls
                else:
                    carry = carry * ls
                    theta = 1.0 + ls * theta
            for p in range(2):
                for k, value in enumerate((e[p], yl[p], sums[p])):
                    for m in range(group):
                        y_send[g * group + m, k, p, q] = value[m * per:(m + 1) * per]

        @pl.when(i == 0)
        def _():
            pl.semaphore_wait(barrier, n + nk - 2)

        for m in range(group):
            to = g * group + m

            @pl.when(to != me)
            def _():
                y_copy(to, me).start()
        return 0

    lax.fori_loop(0, groups, local_group, 0)
    y_recv[me] = y_send[me]

    lam = shift_of(ka * pairs + me * (per * LANES), per)
    lam2 = lam * lam
    unroll = 4 if n % 4 == 0 else 1

    def responses(i, _):
        for d in range(unroll):
            block = i * unroll + d
            for q in range(2):
                s = None
                for j in range(last, -1, -1):
                    row = block * rows + j
                    s, ls, up = row_factors(w_ref, total, q, row, j, last, lam, lam2, s)
                    if j == last:
                        e = s * up
                        yl = e
                        sums = e
                        carry = ls
                        tau = ls
                    else:
                        e = s * (up * e)
                        yl = yl + carry * e
                        sums = sums + (1.0 + tau) * e
                        carry = carry * ls
                        tau = ls * (1.0 + tau)
                for k, value in enumerate((ls, e, carry, yl, tau, sums)):
                    coef[block, k, q] = value
        return 0

    lax.fori_loop(0, n // unroll, responses, 0)

    def y_arrived(k, _):
        y_copy(me, lax.rem(me + k, n)).wait_recv()
        return 0

    lax.fori_loop(1, n, y_arrived, 0)

    zero = jnp.zeros((2, per, LANES), jnp.float32)
    for k in range(3):
        elim[n, k] = zero

    def up_sweep(k, state):
        g = n - 1 - k
        f0, f1, phi, s0, s1, psi = state
        a, b, c, d, alpha, beta = (coef[g, m] for m in range(6))
        inv = 1.0 / (1.0 - d * phi)
        lamb = c * inv
        ls = [(y_recv[g, 1, p] + d * fp) * inv for p, fp in ((0, f0), (1, f1))]
        right = [fp + phi * l for fp, l in ((f0, ls[0]), (f1, ls[1]))]
        new_f = [y_recv[g, 0, p] + b * right[p] for p in range(2)]
        new_s = [y_recv[g, 2, p] + beta * right[p] + sp + psi * ls[p] for p, sp in ((0, s0), (1, s1))]
        new_phi = a + b * (phi * lamb)
        new_psi = alpha + beta * (phi * lamb) + psi * lamb
        elim[g, 0] = new_f[0]
        elim[g, 1] = new_f[1]
        elim[g, 2] = new_phi
        elim[g, 3] = ls[0]
        elim[g, 4] = ls[1]
        elim[g, 5] = lamb
        return new_f[0], new_f[1], new_phi, new_s[0], new_s[1], new_psi

    state = lax.fori_loop(0, n, up_sweep, (zero,) * 6)
    wall = 1.0 / state[5]

    def down_sweep(g, left):
        b_send[g, 0, 0] = left[0]
        b_send[g, 0, 1] = left[1]
        new = [elim[g, 3 + p] + elim[g, 5] * left[p] for p in range(2)]
        for p in range(2):
            b_send[g, 1, p] = elim[g + 1, p] + elim[g + 1, 2] * new[p]

        @pl.when(g != me)
        def _():
            b_copy(g, me).start()

        return new[0], new[1]

    lax.fori_loop(0, n, down_sweep, (-state[3] * wall, -state[4] * wall))
    b_recv[me] = b_send[me]
    sq_buf[...] = jnp.zeros_like(sq_buf)

    def close_group(i, _):
        g = nearest(i, me // group, groups)
        for m in range(group):
            frm = g * group + m

            @pl.when(frm != me)
            def _():
                b_copy(me, frm).wait_recv()

        part = pl.ds(pl.multiple_of(g * count, count), count)
        lam = shift_of(ka * pairs + g * (count * LANES), count)
        kappa = viscous_rate / lam
        joined = lambda k, p, q: jnp.concatenate([b_recv[g * group + m, k, p, q] for m in range(group)], axis=0)
        for q in range(2):
            z = [joined(0, p, q) for p in range(2)]
            after = [joined(1, p, q) for p in range(2)]
            for j in range(rows):
                ls = ls_buf[q, j, part]
                right = r_buf[q, j, part]
                square = None
                for p in range(2):
                    where = (p, q, j // tile, pl.ds(g * span + j % tile, count, stride=tile), slice(None))
                    z[p] = (e_buf[p, q, j, part] + right * after[p]) + ls * z[p]
                    x = z[p] - kappa * f_buf[where]
                    x_buf[where] = x
                    square = x * x if p == 0 else square + x * x
                sq_buf[q, j] += sum(square[m * per:(m + 1) * per] for m in range(group))
        store(i).start()
        return 0

    lax.fori_loop(0, groups, close_group, 0)

    mine[...] = jnp.sum(sq_buf[...], axis=2)

    def s_copy(k):
        return pltpu.make_async_remote_copy(
            src_ref=mine, dst_ref=held.at[k - 1], send_sem=ssend_sem.at[k - 1], recv_sem=srecv_sem.at[k - 1],
            device_id={"ka": lax.rem(ka + k, nk)}, device_id_type=MESH)

    for k in range(1, nk):
        s_copy(k).start()

    def sent(k, _):
        to = lax.rem(me + k, n)
        y_copy(to, me).wait_send()
        b_copy(to, me).wait_send()
        return 0

    lax.fori_loop(1, n, sent, 0)
    added = mine[...]
    for k in range(1, nk):
        s_copy(k).wait_recv()
        added = added + held[k - 1]
    ones = jnp.ones((8, LANES), jnp.float32)
    for q in range(2):
        sums = lax.dot_general(ones, added[q], (((1,), (1,)), ((), ())), precision=lax.Precision.HIGHEST,
                               preferred_element_type=jnp.float32)
        spec_ref[q:q + 1, :] = sums[0:1] * scale
    for k in range(1, nk):
        s_copy(k).wait_send()
    for i in range(groups):
        store(i).wait()


def per_device(n, nk, driving_coefficients):
    _, pairs, _, rows = driving_coefficients.shape
    per = pairs // (LANES * n)
    tile = 8 if rows % 8 == 0 else 1
    cols = pairs // LANES
    group = next((g for g in range(2, n) if n % g == 0 and g * per * tile % 8 == 0), n)
    span = group * per * tile
    f = jnp.transpose(driving_coefficients, (0, 2, 3, 1)).reshape(2, 2, rows // tile, tile, cols, LANES)
    f = jnp.swapaxes(f, 3, 4).reshape(2, 2, rows // tile, cols * tile, LANES)
    table = jnp.asarray(weight_table(n * rows))
    smem = pl.BlockSpec(memory_space=pltpu.SMEM)
    vmem = pl.BlockSpec(memory_space=pltpu.VMEM)
    f32 = jnp.float32
    x, spectrum = pl.pallas_call(
        functools.partial(channel_kernel, n, nk, per, rows, tile, group, 1.0 / (2.0 * pairs * nk)),
        out_shape=(jax.ShapeDtypeStruct(f.shape, f32), jax.ShapeDtypeStruct((2, rows), f32)),
        in_specs=[smem, pl.BlockSpec(memory_space=pl.ANY)],
        out_specs=(pl.BlockSpec(memory_space=pl.ANY), vmem),
        scratch_shapes=[
            pltpu.VMEM(f.shape, f32),
            pltpu.VMEM(f.shape, f32),
            pltpu.VMEM((2, 2, rows, cols, LANES), f32),
            pltpu.VMEM((2, rows, cols, LANES), f32),
            pltpu.VMEM((2, rows, cols, LANES), f32),
            pltpu.VMEM((2, rows, per, LANES), f32),
            pltpu.VMEM((n, 3, 2, 2, per, LANES), f32),
            pltpu.VMEM((n, 3, 2, 2, per, LANES), f32),
            pltpu.VMEM((n, 6, 2, per, LANES), f32),
            pltpu.VMEM((n + 1, 6, 2, per, LANES), f32),
            pltpu.VMEM((n, 2, 2, 2, per, LANES), f32),
            pltpu.VMEM((n, 2, 2, 2, per, LANES), f32),
            pltpu.VMEM((2, rows, LANES), f32),
            pltpu.VMEM((nk - 1, 2, rows, LANES), f32),
            pltpu.SemaphoreType.DMA((n // group,)),
            pltpu.SemaphoreType.DMA((n // group,)),
            pltpu.SemaphoreType.DMA((n,)),
            pltpu.SemaphoreType.DMA((n,)),
            pltpu.SemaphoreType.DMA((n,)),
            pltpu.SemaphoreType.DMA((n,)),
            pltpu.SemaphoreType.DMA((nk - 1,)),
            pltpu.SemaphoreType.DMA((nk - 1,)),
        ],
        compiler_params=pltpu.CompilerParams(collective_id=0, has_side_effects=True),
        name="channel_substep",
    )(table, f)
    x = jnp.swapaxes(x.reshape(2, 2, rows // tile, cols, tile, LANES), 3, 4).reshape(2, 2, rows, pairs)
    return jnp.transpose(x, (0, 3, 1, 2)), spectrum


def solution(mesh):
    n, nk = mesh.shape["gy"], mesh.shape["ka"]
    return jax.shard_map(
        functools.partial(per_device, n, nk), mesh=mesh,
        in_specs=(P(None, "ka", None, "gy"),),
        out_specs=(P(None, "ka", None, "gy"), P(None, "gy")), check_vma=False,
    )
```

```python
import functools

import jax
import jax.numpy as jnp
import numpy as np
from jax import lax
from jax.experimental import pallas as pl
from jax.experimental.pallas import tpu as pltpu
from jax.sharding import PartitionSpec as P

MODES_Z = 512
LANES = 128
MESH = pl.DeviceIdType.MESH

viscous_rate = 400.0
wave_x = 1.0
wave_z = 2.0


def weight_table(total_rows):
    nch = 2 * total_rows
    rows = np.arange(total_rows + 1)
    order = 2 * rows[None, :] + np.arange(2)[:, None]
    top = np.broadcast_to((rows == 0)[None, :], order.shape)
    degree = np.where(top, 4, order).astype(np.float64)
    lower = np.where(order == 2, 2.0, 1.0) / (4.0 * degree * (degree - 1.0))
    middle = np.where(order <= nch - 3, 1.0, 0.0) / (2.0 * (degree * degree - 1.0))
    upper = np.where(order + 2 <= nch - 3, 1.0, 0.0) / (4.0 * degree * (degree + 1.0))
    lower, middle, upper = (np.where(top, 0.0, w) for w in (lower, middle, upper))
    cross = upper[:, :-1] * lower[:, 1:]
    return np.stack([lower[:, :-1], middle[:, :-1], upper[:, :-1], cross]).astype(np.float32).reshape(-1)


def shift_of(first_pair, rows):
    shape = (rows, LANES)
    pair = first_pair + lax.broadcasted_iota(jnp.int32, shape, 0) * LANES + lax.broadcasted_iota(jnp.int32, shape, 1)
    col_x = lax.shift_right_logical(pair, MODES_Z.bit_length() - 1)
    col_z = lax.bitwise_and(pair, MODES_Z - 1)
    signed = jnp.where(col_z < MODES_Z // 2, col_z, col_z - MODES_Z)
    kx = wave_x * col_x.astype(jnp.float32)
    kz = wave_z * signed.astype(jnp.float32)
    return kx * kx + kz * kz + viscous_rate


def row_factors(w_ref, total, q, row, local, last, lam, lam2, s_next):
    at = lambda k: w_ref[(2 * k + q) * total + row]
    pivot = 1.0 + lam * at(1)
    if local < last:
        pivot = pivot - lam2 * at(3) * s_next
    s = 1.0 / pivot
    low = lam * at(0)
    if local == 0:
        low = low + jnp.where(row == 0, 1.0, 0.0)
    return s, low * s, lam * at(2)


def channel_kernel(n, nk, per, rows, tile, group, scale, w_ref, f_hbm, x_hbm, spec_ref,
                   f_buf, x_buf, e_buf, ls_buf, r_buf, sq_buf, both, y_send, y_recv, coef, elim, b_send, edge, mine, held,
                   load_sem, store_sem, dsend_sem, drecv_sem, ysend_sem, yrecv_sem, bsend_sem, erecv_sem, rsend_sem,
                   ssend_sem, srecv_sem):
    total = n * rows
    last = rows - 1
    me = lax.axis_index("gy")
    ka = lax.axis_index("ka")
    pairs = n * per * LANES
    count = group * per
    span = count * tile
    groups = n // group
    chips = n // 2
    chip, core = me // 2, lax.rem(me, 2)
    sibling = 2 * chip + 1 - core

    def nearest(k, here, size):
        return lax.bitwise_xor(here, k) if size & (size - 1) == 0 else lax.rem(here + k, size)

    def load(i):
        g = nearest(groups - 1 - i, me // group, groups)
        where = pl.ds(pl.multiple_of(g * span, span), span)
        return pltpu.make_async_copy(f_hbm.at[:, :, :, where, :], f_buf.at[:, :, :, where, :], load_sem.at[i])

    def store(i):
        g = nearest(i, me // group, groups)
        where = pl.ds(pl.multiple_of(g * span, span), span)
        return pltpu.make_async_copy(x_buf.at[:, :, :, where, :], x_hbm.at[:, :, :, where, :], store_sem.at[i])

    for i in range(groups):
        load(i).start()

    barrier = pltpu.get_barrier_semaphore()

    def greet(k, _):
        pl.semaphore_signal(barrier, inc=1, device_id={"gy": lax.rem(me + k, n)}, device_id_type=MESH)
        return 0

    lax.fori_loop(1, n, greet, 0)
    for k in range(1, nk):
        pl.semaphore_signal(barrier, inc=1, device_id={"ka": lax.rem(ka + k, nk)}, device_id_type=MESH)

    def d_copy(which, g):
        where = pl.ds(g * group, group)
        return pltpu.make_async_remote_copy(
            src_ref=both.at[which, where], dst_ref=both.at[which, where], send_sem=dsend_sem.at[g],
            recv_sem=drecv_sem.at[g], device_id={"gy": sibling}, device_id_type=MESH)

    def y_copy(to, frm):
        return pltpu.make_async_remote_copy(
            src_ref=y_send.at[to], dst_ref=y_recv.at[frm], send_sem=ysend_sem.at[to],
            recv_sem=yrecv_sem.at[frm], device_id={"gy": 2 * to + core}, device_id_type=MESH)

    def b_copy(to, owner):
        return pltpu.make_async_remote_copy(
            src_ref=b_send.at[to], dst_ref=edge.at[owner], send_sem=bsend_sem.at[to],
            recv_sem=erecv_sem.at[owner], device_id={"gy": 2 * to + core}, device_id_type=MESH)

    def r_copy(owner):
        return pltpu.make_async_remote_copy(
            src_ref=edge.at[owner], dst_ref=edge.at[owner], send_sem=rsend_sem.at[owner // 2],
            recv_sem=erecv_sem.at[owner], device_id={"gy": sibling}, device_id_type=MESH)

    def local_group(i):
        g = nearest(groups - 1 - i, me // group, groups)
        load(i).wait()
        part = pl.ds(pl.multiple_of(g * count, count), count)
        lam = shift_of(ka * pairs + g * (count * LANES), count)
        lam2 = lam * lam
        kappa = viscous_rate / lam
        for q in range(2):
            s = None
            e = [None, None]
            yl = [None, None]
            sums = [None, None]
            for j in range(last, -1, -1):
                row = me * rows + j
                s, ls, up = row_factors(w_ref, total, q, row, j, last, lam, lam2, s)
                right = s * up if j == last else (s * up) * right
                ls_buf[q, j, part] = ls
                r_buf[q, j, part] = right
                for p in range(2):
                    f = f_buf[p, q, j // tile, pl.ds(g * span + j % tile, count, stride=tile), :]
                    src = kappa * f
                    if j == last:
                        e[p] = s * src
                        yl[p] = e[p]
                        sums[p] = e[p] - src
                    else:
                        e[p] = s * (src + up * e[p])
                        yl[p] = yl[p] + carry * e[p]
                        sums[p] = sums[p] + (theta * e[p] - src)
                    e_buf[p, q, j, part] = e[p]
                if j == last:
                    end, beta = right, right
                    carry = ls
                    tau = ls
                else:
                    end = end + carry * right
                    beta = beta + theta * right
                    carry = carry * ls
                    tau = ls * theta
                theta = 1.0 + tau
            for k, value in enumerate((*e, *yl, *sums, ls, right, carry, end, tau, beta)):
                for m in range(group):
                    both[core, g * group + m, k, q] = value[m * per:(m + 1) * per]

        @pl.when(i == 0)
        def _():
            pl.semaphore_wait(barrier, n + nk - 2)

        d_copy(core, g).start()

    def combine_group(i):
        g = nearest(groups - 1 - i, me // group, groups)
        d_copy(1 - core, g).wait_recv()
        for m in range(group // 2):
            to = g * (group // 2) + m
            chunk = 2 * to + core
            low = [both[0, chunk, k] for k in range(12)]
            high = [both[1, chunk, k] for k in range(12)]
            inv = 1.0 / (1.0 - low[9] * high[6])
            for p in range(2):
                below = inv * (low[2 + p] + low[9] * high[p])
                above = high[p] + high[6] * below
                y_send[to, 0, p] = low[p] + low[7] * above
                y_send[to, 1, p] = high[2 + p] + high[8] * below
                y_send[to, 2, p] = (low[4 + p] + high[4 + p]) + (low[11] * above + high[10] * below)

            @pl.when(to != chip)
            def _():
                y_copy(to, chip).start()

    def up_phase(i, _):
        @pl.when(i < groups)
        def _():
            local_group(i)

        @pl.when(i > 0)
        def _():
            combine_group(i - 1)

        return 0

    lax.fori_loop(0, groups + 1, up_phase, 0)
    y_recv[chip] = y_send[chip]

    lam = shift_of(ka * pairs + me * (per * LANES), per)
    lam2 = lam * lam
    unroll = 4 if n % 4 == 0 else 1

    def responses(i, _):
        for d in range(unroll):
            block = i * unroll + d
            for q in range(2):
                s = None
                for j in range(last, -1, -1):
                    row = block * rows + j
                    s, ls, up = row_factors(w_ref, total, q, row, j, last, lam, lam2, s)
                    if j == last:
                        e = s * up
                        yl = e
                        sums = e
                        carry = ls
                        tau = ls
                    else:
                        e = s * (up * e)
                        yl = yl + carry * e
                        sums = sums + (1.0 + tau) * e
                        carry = carry * ls
                        tau = ls * (1.0 + tau)
                for k, value in enumerate((ls, e, carry, yl, tau, sums)):
                    coef[block, k, q] = value
        return 0

    lax.fori_loop(0, n // unroll, responses, 0)

    def chip_responses(c, _):
        a0, b0, c0, d0, alpha0, beta0 = (coef[2 * c, k] for k in range(6))
        a1, b1, c1, d1, alpha1, beta1 = (coef[2 * c + 1, k] for k in range(6))
        inv = 1.0 / (1.0 - d0 * a1)
        low_left, low_right = inv * c0, inv * d0 * b1
        high_left, high_right = a1 * low_left, b1 * inv
        for k, value in enumerate((a0 + b0 * high_left, b0 * high_right, c1 * low_left, d1 + c1 * low_right,
                                   alpha0 + beta0 * high_left + alpha1 * low_left,
                                   beta1 + beta0 * high_right + alpha1 * low_right)):
            coef[c, k] = value
        return 0

    lax.fori_loop(0, chips, chip_responses, 0)

    def y_arrived(k, _):
        y_copy(chip, lax.rem(chip + k, chips)).wait_recv()
        return 0

    lax.fori_loop(1, chips, y_arrived, 0)

    zero = jnp.zeros((2, per, LANES), jnp.float32)
    for k in range(3):
        elim[chips, k] = zero

    def up_sweep(k, state):
        g = chips - 1 - k
        f0, f1, phi, s0, s1, psi = state
        a, b, c, d, alpha, beta = (coef[g, m] for m in range(6))
        inv = 1.0 / (1.0 - d * phi)
        lamb = c * inv
        ls = [(y_recv[g, 1, p] + d * fp) * inv for p, fp in ((0, f0), (1, f1))]
        right = [fp + phi * l for fp, l in ((f0, ls[0]), (f1, ls[1]))]
        new_f = [y_recv[g, 0, p] + b * right[p] for p in range(2)]
        new_s = [y_recv[g, 2, p] + beta * right[p] + sp + psi * ls[p] for p, sp in ((0, s0), (1, s1))]
        new_phi = a + b * (phi * lamb)
        new_psi = alpha + beta * (phi * lamb) + psi * lamb
        elim[g, 0] = new_f[0]
        elim[g, 1] = new_f[1]
        elim[g, 2] = new_phi
        elim[g, 3] = ls[0]
        elim[g, 4] = ls[1]
        elim[g, 5] = lamb
        return new_f[0], new_f[1], new_phi, new_s[0], new_s[1], new_psi

    state = lax.fori_loop(0, chips, up_sweep, (zero,) * 6)
    wall = 1.0 / state[5]

    def down_sweep(g, left):
        b_send[g, 0, 0] = left[0]
        b_send[g, 0, 1] = left[1]
        new = [elim[g, 3 + p] + elim[g, 5] * left[p] for p in range(2)]
        for p in range(2):
            b_send[g, 1, p] = elim[g + 1, p] + elim[g + 1, 2] * new[p]

        @pl.when(g != chip)
        def _():
            b_copy(g, me).start()

        return new[0], new[1]

    lax.fori_loop(0, chips, down_sweep, (-state[3] * wall, -state[4] * wall))
    edge[me] = b_send[chip]
    sq_buf[...] = jnp.zeros_like(sq_buf)

    def relay_group(i):
        g = nearest(i, me // group, groups)
        for m in range(group // 2):
            owner = g * group + 2 * m + core

            @pl.when(owner != me)
            def _():
                b_copy(chip, owner).wait_recv()

            r_copy(owner).start()

    def close_group(i):
        g = nearest(i, me // group, groups)
        for m in range(group // 2):
            r_copy(g * group + 2 * m + 1 - core).wait_recv()
        part = pl.ds(pl.multiple_of(g * count, count), count)
        lam = shift_of(ka * pairs + g * (count * LANES), count)
        kappa = viscous_rate / lam
        joined = lambda get: jnp.concatenate([get(g * group + m) for m in range(group)], axis=0)
        for q in range(2):
            low = [joined(lambda c: both[0, c, k, q]) for k in range(12)]
            high = [joined(lambda c: both[1, c, k, q]) for k in range(12)]
            inv = 1.0 / (1.0 - low[9] * high[6])
            z, after = [], []
            for p in range(2):
                outer_left = joined(lambda c: edge[c, 0, p, q])
                outer_right = joined(lambda c: edge[c, 1, p, q])
                below = inv * (low[2 + p] + low[9] * (high[p] + high[7] * outer_right) + low[8] * outer_left)
                above = high[p] + high[6] * below + high[7] * outer_right
                z.append(jnp.where(core == 0, outer_left, below))
                after.append(jnp.where(core == 0, above, outer_right))
            for j in range(rows):
                ls = ls_buf[q, j, part]
                right = r_buf[q, j, part]
                square = None
                for p in range(2):
                    where = (p, q, j // tile, pl.ds(g * span + j % tile, count, stride=tile), slice(None))
                    z[p] = (e_buf[p, q, j, part] + right * after[p]) + ls * z[p]
                    x = z[p] - kappa * f_buf[where]
                    x_buf[where] = x
                    square = x * x if p == 0 else square + x * x
                sq_buf[q, j] += sum(square[m * per:(m + 1) * per] for m in range(group))
        store(i).start()

    def down_phase(i, _):
        @pl.when(i < groups)
        def _():
            relay_group(i)

        @pl.when(i > 0)
        def _():
            close_group(i - 1)

        return 0

    lax.fori_loop(0, groups + 1, down_phase, 0)

    mine[...] = jnp.sum(sq_buf[...], axis=2)

    def s_copy(k):
        return pltpu.make_async_remote_copy(
            src_ref=mine, dst_ref=held.at[k - 1], send_sem=ssend_sem.at[k - 1], recv_sem=srecv_sem.at[k - 1],
            device_id={"ka": lax.rem(ka + k, nk)}, device_id_type=MESH)

    for k in range(1, nk):
        s_copy(k).start()

    def sent(k, _):
        to = lax.rem(chip + k, chips)
        y_copy(to, chip).wait_send()
        b_copy(to, me).wait_send()
        return 0

    lax.fori_loop(1, chips, sent, 0)

    def relayed(c, _):
        r_copy(2 * c + core).wait_send()
        return 0

    lax.fori_loop(0, chips, relayed, 0)

    def given(g, _):
        d_copy(core, g).wait_send()
        return 0

    lax.fori_loop(0, groups, given, 0)
    added = mine[...]
    for k in range(1, nk):
        s_copy(k).wait_recv()
        added = added + held[k - 1]
    ones = jnp.ones((8, LANES), jnp.float32)
    for q in range(2):
        sums = lax.dot_general(ones, added[q], (((1,), (1,)), ((), ())), precision=lax.Precision.HIGHEST,
                               preferred_element_type=jnp.float32)
        spec_ref[q:q + 1, :] = sums[0:1] * scale
    for k in range(1, nk):
        s_copy(k).wait_send()
    for i in range(groups):
        store(i).wait()


def per_device(n, nk, driving_coefficients):
    _, pairs, _, rows = driving_coefficients.shape
    per = pairs // (LANES * n)
    tile = 8 if rows % 8 == 0 else 1
    cols = pairs // LANES
    chips = n // 2
    group = next((g for g in range(2, n) if n % g == 0 and g * per * tile % 8 == 0), n)
    span = group * per * tile
    f = jnp.transpose(driving_coefficients, (0, 2, 3, 1)).reshape(2, 2, rows // tile, tile, cols, LANES)
    f = jnp.swapaxes(f, 3, 4).reshape(2, 2, rows // tile, cols * tile, LANES)
    table = jnp.asarray(weight_table(n * rows))
    smem = pl.BlockSpec(memory_space=pltpu.SMEM)
    vmem = pl.BlockSpec(memory_space=pltpu.VMEM)
    f32 = jnp.float32
    x, spectrum = pl.pallas_call(
        functools.partial(channel_kernel, n, nk, per, rows, tile, group, 1.0 / (2.0 * pairs * nk)),
        out_shape=(jax.ShapeDtypeStruct(f.shape, f32), jax.ShapeDtypeStruct((2, rows), f32)),
        in_specs=[smem, pl.BlockSpec(memory_space=pl.ANY)],
        out_specs=(pl.BlockSpec(memory_space=pl.ANY), vmem),
        scratch_shapes=[
            pltpu.VMEM(f.shape, f32),
            pltpu.VMEM(f.shape, f32),
            pltpu.VMEM((2, 2, rows, cols, LANES), f32),
            pltpu.VMEM((2, rows, cols, LANES), f32),
            pltpu.VMEM((2, rows, cols, LANES), f32),
            pltpu.VMEM((2, rows, per, LANES), f32),
            pltpu.VMEM((2, n, 12, 2, per, LANES), f32),
            pltpu.VMEM((chips, 3, 2, 2, per, LANES), f32),
            pltpu.VMEM((chips, 3, 2, 2, per, LANES), f32),
            pltpu.VMEM((n, 6, 2, per, LANES), f32),
            pltpu.VMEM((chips + 1, 6, 2, per, LANES), f32),
            pltpu.VMEM((chips, 2, 2, 2, per, LANES), f32),
            pltpu.VMEM((n, 2, 2, 2, per, LANES), f32),
            pltpu.VMEM((2, rows, LANES), f32),
            pltpu.VMEM((nk - 1, 2, rows, LANES), f32),
            *[pltpu.SemaphoreType.DMA((n // group,))] * 4,
            *[pltpu.SemaphoreType.DMA((chips,))] * 3,
            pltpu.SemaphoreType.DMA((n,)),
            pltpu.SemaphoreType.DMA((chips,)),
            pltpu.SemaphoreType.DMA((nk - 1,)),
            pltpu.SemaphoreType.DMA((nk - 1,)),
        ],
        compiler_params=pltpu.CompilerParams(collective_id=0, has_side_effects=True),
        name="channel_substep",
    )(table, f)
    x = jnp.swapaxes(x.reshape(2, 2, rows // tile, cols, tile, LANES), 3, 4).reshape(2, 2, rows, pairs)
    return jnp.transpose(x, (0, 3, 1, 2)), spectrum


def solution(mesh):
    n, nk = mesh.shape["gy"], mesh.shape["ka"]
    return jax.shard_map(
        functools.partial(per_device, n, nk), mesh=mesh,
        in_specs=(P(None, "ka", None, "gy"),),
        out_specs=(P(None, "ka", None, "gy"), P(None, "gy")), check_vma=False,
    )
```

```python
import functools

import jax
import jax.numpy as jnp
import numpy as np
from jax import lax
from jax.experimental import pallas as pl
from jax.experimental.pallas import tpu as pltpu
from jax.sharding import PartitionSpec as P

MODES_Z = 512
LANES = 128
MESH = pl.DeviceIdType.MESH

viscous_rate = 400.0
wave_x = 1.0
wave_z = 2.0


def weight_table(total_rows):
    nch = 2 * total_rows
    rows = np.arange(total_rows + 1)
    order = 2 * rows[None, :] + np.arange(2)[:, None]
    top = np.broadcast_to((rows == 0)[None, :], order.shape)
    degree = np.where(top, 4, order).astype(np.float64)
    lower = np.where(order == 2, 2.0, 1.0) / (4.0 * degree * (degree - 1.0))
    middle = np.where(order <= nch - 3, 1.0, 0.0) / (2.0 * (degree * degree - 1.0))
    upper = np.where(order + 2 <= nch - 3, 1.0, 0.0) / (4.0 * degree * (degree + 1.0))
    lower, middle, upper = (np.where(top, 0.0, w) for w in (lower, middle, upper))
    cross = upper[:, :-1] * lower[:, 1:]
    return np.stack([lower[:, :-1], middle[:, :-1], upper[:, :-1], cross]).astype(np.float32).reshape(-1)


def shift_of(first_pair, rows):
    shape = (rows, LANES)
    pair = first_pair + lax.broadcasted_iota(jnp.int32, shape, 0) * LANES + lax.broadcasted_iota(jnp.int32, shape, 1)
    col_x = lax.shift_right_logical(pair, MODES_Z.bit_length() - 1)
    col_z = lax.bitwise_and(pair, MODES_Z - 1)
    signed = jnp.where(col_z < MODES_Z // 2, col_z, col_z - MODES_Z)
    kx = wave_x * col_x.astype(jnp.float32)
    kz = wave_z * signed.astype(jnp.float32)
    return kx * kx + kz * kz + viscous_rate


def row_factors(w_ref, total, q, row, local, last, lam, lam2, s_next):
    at = lambda k: w_ref[(2 * k + q) * total + row]
    pivot = 1.0 + lam * at(1)
    if local < last:
        pivot = pivot - lam2 * at(3) * s_next
    s = 1.0 / pivot
    low = lam * at(0)
    if local == 0:
        low = low + jnp.where(row == 0, 1.0, 0.0)
    return s, low * s, lam * at(2)


def channel_kernel(n, nk, per, rows, tile, group, scale, w_hbm, f_hbm, x_buf, spec_ref,
                   w_ref, f_buf, e_buf, ls_buf, r_buf, sq_buf, both, y_send, y_recv, coef, elim, b_send, edge, mine, held,
                   table_sem, load_sem, dsend_sem, drecv_sem, ysend_sem, yrecv_sem, bsend_sem, erecv_sem, rsend_sem,
                   ssend_sem, srecv_sem):
    total = n * rows
    last = rows - 1
    me = lax.axis_index("gy")
    ka = lax.axis_index("ka")
    pairs = n * per * LANES
    count = group * per
    span = count * tile
    groups = n // group
    chips = n // 2
    chip, core = me // 2, lax.rem(me, 2)
    sibling = 2 * chip + 1 - core

    def nearest(k, here, size):
        return lax.bitwise_xor(here, k) if size & (size - 1) == 0 else lax.rem(here + k, size)

    def load(i):
        g = nearest(groups - 1 - i, me // group, groups)
        where = pl.ds(pl.multiple_of(g * span, span), span)
        return pltpu.make_async_copy(f_hbm.at[:, :, :, where, :], f_buf.at[:, :, :, where, :], load_sem.at[i])

    table = pltpu.make_async_copy(w_hbm, w_ref, table_sem)
    table.start()
    for i in range(groups):
        load(i).start()

    barrier = pltpu.get_barrier_semaphore()

    def greet(k, _):
        pl.semaphore_signal(barrier, inc=1, device_id={"gy": lax.rem(me + k, n)}, device_id_type=MESH)
        return 0

    lax.fori_loop(1, n, greet, 0)
    for k in range(1, nk):
        pl.semaphore_signal(barrier, inc=1, device_id={"ka": lax.rem(ka + k, nk)}, device_id_type=MESH)

    def d_copy(which, g):
        where = pl.ds(g * group, group)
        return pltpu.make_async_remote_copy(
            src_ref=both.at[which, where], dst_ref=both.at[which, where], send_sem=dsend_sem.at[g],
            recv_sem=drecv_sem.at[g], device_id={"gy": sibling}, device_id_type=MESH)

    def y_copy(to, frm):
        return pltpu.make_async_remote_copy(
            src_ref=y_send.at[to], dst_ref=y_recv.at[frm], send_sem=ysend_sem.at[to],
            recv_sem=yrecv_sem.at[frm], device_id={"gy": 2 * to + core}, device_id_type=MESH)

    def b_copy(to, owner):
        return pltpu.make_async_remote_copy(
            src_ref=b_send.at[to], dst_ref=edge.at[owner], send_sem=bsend_sem.at[to],
            recv_sem=erecv_sem.at[owner], device_id={"gy": 2 * to + core}, device_id_type=MESH)

    def r_copy(owner):
        return pltpu.make_async_remote_copy(
            src_ref=edge.at[owner], dst_ref=edge.at[owner], send_sem=rsend_sem.at[owner // 2],
            recv_sem=erecv_sem.at[owner], device_id={"gy": sibling}, device_id_type=MESH)

    def local_group(i):
        g = nearest(groups - 1 - i, me // group, groups)
        load(i).wait()
        part = pl.ds(pl.multiple_of(g * count, count), count)
        lam = shift_of(ka * pairs + g * (count * LANES), count)
        lam2 = lam * lam
        kappa = viscous_rate / lam
        for q in range(2):
            s = None
            e = [None, None]
            yl = [None, None]
            sums = [None, None]
            for j in range(last, -1, -1):
                row = me * rows + j
                s, ls, up = row_factors(w_ref, total, q, row, j, last, lam, lam2, s)
                right = s * up if j == last else (s * up) * right
                ls_buf[q, j, part] = ls
                r_buf[q, j, part] = right
                for p in range(2):
                    f = f_buf[p, q, j // tile, pl.ds(g * span + j % tile, count, stride=tile), :]
                    src = kappa * f
                    if j == last:
                        e[p] = s * src
                        yl[p] = e[p]
                        sums[p] = e[p] - src
                    else:
                        e[p] = s * (src + up * e[p])
                        yl[p] = yl[p] + carry * e[p]
                        sums[p] = sums[p] + (theta * e[p] - src)
                    e_buf[p, q, j, part] = e[p]
                if j == last:
                    end, beta = right, right
                    carry = ls
                    tau = ls
                else:
                    end = end + carry * right
                    beta = beta + theta * right
                    carry = carry * ls
                    tau = ls * theta
                theta = 1.0 + tau
            for k, value in enumerate((*e, *yl, *sums, ls, right, carry, end, tau, beta)):
                for m in range(group):
                    both[core, g * group + m, k, q] = value[m * per:(m + 1) * per]

        @pl.when(i == 0)
        def _():
            pl.semaphore_wait(barrier, n + nk - 2)

        d_copy(core, g).start()

    def combine_group(i):
        g = nearest(groups - 1 - i, me // group, groups)
        d_copy(1 - core, g).wait_recv()
        for m in range(group // 2):
            to = g * (group // 2) + m
            chunk = 2 * to + core
            low = [both[0, chunk, k] for k in range(12)]
            high = [both[1, chunk, k] for k in range(12)]
            inv = 1.0 / (1.0 - low[9] * high[6])
            for p in range(2):
                below = inv * (low[2 + p] + low[9] * high[p])
                above = high[p] + high[6] * below
                y_send[to, 0, p] = low[p] + low[7] * above
                y_send[to, 1, p] = high[2 + p] + high[8] * below
                y_send[to, 2, p] = (low[4 + p] + high[4 + p]) + (low[11] * above + high[10] * below)

            @pl.when(to != chip)
            def _():
                y_copy(to, chip).start()

    table.wait()

    def up_phase(i, _):
        @pl.when(i < groups)
        def _():
            local_group(i)

        @pl.when(i > 0)
        def _():
            combine_group(i - 1)

        return 0

    lax.fori_loop(0, groups + 1, up_phase, 0)
    y_recv[chip] = y_send[chip]

    lam = shift_of(ka * pairs + me * (per * LANES), per)
    lam2 = lam * lam
    unroll = 4 if n % 4 == 0 else 1

    def responses(i, _):
        for d in range(unroll):
            block = i * unroll + d
            for q in range(2):
                s = None
                for j in range(last, -1, -1):
                    row = block * rows + j
                    s, ls, up = row_factors(w_ref, total, q, row, j, last, lam, lam2, s)
                    if j == last:
                        e = s * up
                        yl = e
                        sums = e
                        carry = ls
                        tau = ls
                    else:
                        e = s * (up * e)
                        yl = yl + carry * e
                        sums = sums + (1.0 + tau) * e
                        carry = carry * ls
                        tau = ls * (1.0 + tau)
                for k, value in enumerate((ls, e, carry, yl, tau, sums)):
                    coef[block, k, q] = value
        return 0

    lax.fori_loop(0, n // unroll, responses, 0)

    def chip_responses(c, _):
        a0, b0, c0, d0, alpha0, beta0 = (coef[2 * c, k] for k in range(6))
        a1, b1, c1, d1, alpha1, beta1 = (coef[2 * c + 1, k] for k in range(6))
        inv = 1.0 / (1.0 - d0 * a1)
        low_left, low_right = inv * c0, inv * d0 * b1
        high_left, high_right = a1 * low_left, b1 * inv
        for k, value in enumerate((a0 + b0 * high_left, b0 * high_right, c1 * low_left, d1 + c1 * low_right,
                                   alpha0 + beta0 * high_left + alpha1 * low_left,
                                   beta1 + beta0 * high_right + alpha1 * low_right)):
            coef[c, k] = value
        return 0

    lax.fori_loop(0, chips, chip_responses, 0)

    def y_arrived(k, _):
        y_copy(chip, lax.rem(chip + k, chips)).wait_recv()
        return 0

    lax.fori_loop(1, chips, y_arrived, 0)

    zero = jnp.zeros((2, per, LANES), jnp.float32)
    for k in range(3):
        elim[chips, k] = zero

    def up_sweep(k, state):
        g = chips - 1 - k
        f0, f1, phi, s0, s1, psi = state
        a, b, c, d, alpha, beta = (coef[g, m] for m in range(6))
        inv = 1.0 / (1.0 - d * phi)
        lamb = c * inv
        ls = [(y_recv[g, 1, p] + d * fp) * inv for p, fp in ((0, f0), (1, f1))]
        right = [fp + phi * l for fp, l in ((f0, ls[0]), (f1, ls[1]))]
        new_f = [y_recv[g, 0, p] + b * right[p] for p in range(2)]
        new_s = [y_recv[g, 2, p] + beta * right[p] + sp + psi * ls[p] for p, sp in ((0, s0), (1, s1))]
        new_phi = a + b * (phi * lamb)
        new_psi = alpha + beta * (phi * lamb) + psi * lamb
        elim[g, 0] = new_f[0]
        elim[g, 1] = new_f[1]
        elim[g, 2] = new_phi
        elim[g, 3] = ls[0]
        elim[g, 4] = ls[1]
        elim[g, 5] = lamb
        return new_f[0], new_f[1], new_phi, new_s[0], new_s[1], new_psi

    state = lax.fori_loop(0, chips, up_sweep, (zero,) * 6)
    wall = 1.0 / state[5]

    def down_sweep(g, left):
        b_send[g, 0, 0] = left[0]
        b_send[g, 0, 1] = left[1]
        new = [elim[g, 3 + p] + elim[g, 5] * left[p] for p in range(2)]
        for p in range(2):
            b_send[g, 1, p] = elim[g + 1, p] + elim[g + 1, 2] * new[p]

        @pl.when(g != chip)
        def _():
            b_copy(g, me).start()

        return new[0], new[1]

    lax.fori_loop(0, chips, down_sweep, (-state[3] * wall, -state[4] * wall))
    edge[me] = b_send[chip]
    sq_buf[...] = jnp.zeros_like(sq_buf)

    def relay_group(i):
        g = nearest(i, me // group, groups)
        for m in range(group // 2):
            owner = g * group + 2 * m + core

            @pl.when(owner != me)
            def _():
                b_copy(chip, owner).wait_recv()

            r_copy(owner).start()

    def close_group(i):
        g = nearest(i, me // group, groups)
        for m in range(group // 2):
            r_copy(g * group + 2 * m + 1 - core).wait_recv()
        part = pl.ds(pl.multiple_of(g * count, count), count)
        lam = shift_of(ka * pairs + g * (count * LANES), count)
        kappa = viscous_rate / lam
        joined = lambda get: jnp.concatenate([get(g * group + m) for m in range(group)], axis=0)
        for q in range(2):
            low = [joined(lambda c: both[0, c, k, q]) for k in range(12)]
            high = [joined(lambda c: both[1, c, k, q]) for k in range(12)]
            inv = 1.0 / (1.0 - low[9] * high[6])
            z, after = [], []
            for p in range(2):
                outer_left = joined(lambda c: edge[c, 0, p, q])
                outer_right = joined(lambda c: edge[c, 1, p, q])
                below = inv * (low[2 + p] + low[9] * (high[p] + high[7] * outer_right) + low[8] * outer_left)
                above = high[p] + high[6] * below + high[7] * outer_right
                z.append(jnp.where(core == 0, outer_left, below))
                after.append(jnp.where(core == 0, above, outer_right))
            for j in range(rows):
                ls = ls_buf[q, j, part]
                right = r_buf[q, j, part]
                square = None
                for p in range(2):
                    where = (p, q, j // tile, pl.ds(g * span + j % tile, count, stride=tile), slice(None))
                    z[p] = (e_buf[p, q, j, part] + right * after[p]) + ls * z[p]
                    x = z[p] - kappa * f_buf[where]
                    x_buf[where] = x
                    square = x * x if p == 0 else square + x * x
                sq_buf[q, j] += sum(square[m * per:(m + 1) * per] for m in range(group))

    def down_phase(i, _):
        @pl.when(i < groups)
        def _():
            relay_group(i)

        @pl.when(i > 0)
        def _():
            close_group(i - 1)

        return 0

    lax.fori_loop(0, groups + 1, down_phase, 0)

    mine[...] = jnp.sum(sq_buf[...], axis=2)

    def s_copy(k):
        return pltpu.make_async_remote_copy(
            src_ref=mine, dst_ref=held.at[k - 1], send_sem=ssend_sem.at[k - 1], recv_sem=srecv_sem.at[k - 1],
            device_id={"ka": lax.rem(ka + k, nk)}, device_id_type=MESH)

    for k in range(1, nk):
        s_copy(k).start()

    def sent(k, _):
        to = lax.rem(chip + k, chips)
        y_copy(to, chip).wait_send()
        b_copy(to, me).wait_send()
        return 0

    lax.fori_loop(1, chips, sent, 0)

    def relayed(c, _):
        r_copy(2 * c + core).wait_send()
        return 0

    lax.fori_loop(0, chips, relayed, 0)

    def given(g, _):
        d_copy(core, g).wait_send()
        return 0

    lax.fori_loop(0, groups, given, 0)
    added = mine[...]
    for k in range(1, nk):
        s_copy(k).wait_recv()
        added = added + held[k - 1]
    ones = jnp.ones((8, LANES), jnp.float32)
    for q in range(2):
        sums = lax.dot_general(ones, added[q], (((1,), (1,)), ((), ())), precision=lax.Precision.HIGHEST,
                               preferred_element_type=jnp.float32)
        spec_ref[q:q + 1, :] = sums[0:1] * scale
    for k in range(1, nk):
        s_copy(k).wait_send()


def per_device(n, nk, driving_coefficients):
    _, pairs, _, rows = driving_coefficients.shape
    per = pairs // (LANES * n)
    tile = 8 if rows % 8 == 0 else 1
    cols = pairs // LANES
    chips = n // 2
    group = next((g for g in range(2, n) if n % g == 0 and g * per * tile % 8 == 0), n)
    span = group * per * tile
    f = jnp.transpose(driving_coefficients, (0, 2, 3, 1)).reshape(2, 2, rows // tile, tile, cols, LANES)
    f = jnp.swapaxes(f, 3, 4).reshape(2, 2, rows // tile, cols * tile, LANES)
    table = jnp.asarray(weight_table(n * rows))
    vmem = pl.BlockSpec(memory_space=pltpu.VMEM)
    f32 = jnp.float32
    x, spectrum = pl.pallas_call(
        functools.partial(channel_kernel, n, nk, per, rows, tile, group, 1.0 / (2.0 * pairs * nk)),
        out_shape=(jax.ShapeDtypeStruct(f.shape, f32), jax.ShapeDtypeStruct((2, rows), f32)),
        in_specs=[pl.BlockSpec(memory_space=pltpu.HBM)] * 2,
        out_specs=(vmem, vmem),
        scratch_shapes=[
            pltpu.SMEM(table.shape, f32),
            pltpu.VMEM(f.shape, f32),
            pltpu.VMEM((2, 2, rows, cols, LANES), f32),
            pltpu.VMEM((2, rows, cols, LANES), f32),
            pltpu.VMEM((2, rows, cols, LANES), f32),
            pltpu.VMEM((2, rows, per, LANES), f32),
            pltpu.VMEM((2, n, 12, 2, per, LANES), f32),
            pltpu.VMEM((chips, 3, 2, 2, per, LANES), f32),
            pltpu.VMEM((chips, 3, 2, 2, per, LANES), f32),
            pltpu.VMEM((n, 6, 2, per, LANES), f32),
            pltpu.VMEM((chips + 1, 6, 2, per, LANES), f32),
            pltpu.VMEM((chips, 2, 2, 2, per, LANES), f32),
            pltpu.VMEM((n, 2, 2, 2, per, LANES), f32),
            pltpu.VMEM((2, rows, LANES), f32),
            pltpu.VMEM((nk - 1, 2, rows, LANES), f32),
            pltpu.SemaphoreType.DMA,
            *[pltpu.SemaphoreType.DMA((n // group,))] * 3,
            *[pltpu.SemaphoreType.DMA((chips,))] * 3,
            pltpu.SemaphoreType.DMA((n,)),
            pltpu.SemaphoreType.DMA((chips,)),
            pltpu.SemaphoreType.DMA((nk - 1,)),
            pltpu.SemaphoreType.DMA((nk - 1,)),
        ],
        compiler_params=pltpu.CompilerParams(collective_id=0, has_side_effects=True, vmem_limit_bytes=24 << 20),
        name="channel_substep",
    )(*(pltpu.with_memory_space_constraint(given, pltpu.HBM) for given in (table, f)))
    x = jnp.swapaxes(x.reshape(2, 2, rows // tile, cols, tile, LANES), 3, 4).reshape(2, 2, rows, pairs)
    return jnp.transpose(x, (0, 3, 1, 2)), spectrum


def solution(mesh):
    n, nk = mesh.shape["gy"], mesh.shape["ka"]
    return jax.shard_map(
        functools.partial(per_device, n, nk), mesh=mesh,
        in_specs=(P(None, "ka", None, "gy"),),
        out_specs=(P(None, "ka", None, "gy"), P(None, "gy")), check_vma=False,
    )
```

```python
import functools

import jax
import jax.numpy as jnp
import numpy as np
from jax import lax
from jax.experimental import pallas as pl
from jax.experimental.pallas import tpu as pltpu
from jax.sharding import PartitionSpec as P

MODES_Z = 512
LANES = 128
MESH = pl.DeviceIdType.MESH

viscous_rate = 400.0
wave_x = 1.0
wave_z = 2.0


def weight_table(total_rows):
    nch = 2 * total_rows
    rows = np.arange(total_rows + 1)
    order = 2 * rows[None, :] + np.arange(2)[:, None]
    top = np.broadcast_to((rows == 0)[None, :], order.shape)
    degree = np.where(top, 4, order).astype(np.float64)
    lower = np.where(order == 2, 2.0, 1.0) / (4.0 * degree * (degree - 1.0))
    middle = np.where(order <= nch - 3, 1.0, 0.0) / (2.0 * (degree * degree - 1.0))
    upper = np.where(order + 2 <= nch - 3, 1.0, 0.0) / (4.0 * degree * (degree + 1.0))
    lower, middle, upper = (np.where(top, 0.0, w) for w in (lower, middle, upper))
    cross = upper[:, :-1] * lower[:, 1:]
    return np.stack([lower[:, :-1], middle[:, :-1], upper[:, :-1], cross]).astype(np.float32).reshape(-1)


def shift_of(first_pair, rows):
    shape = (rows, LANES)
    pair = first_pair + lax.broadcasted_iota(jnp.int32, shape, 0) * LANES + lax.broadcasted_iota(jnp.int32, shape, 1)
    col_x = lax.shift_right_logical(pair, MODES_Z.bit_length() - 1)
    col_z = lax.bitwise_and(pair, MODES_Z - 1)
    signed = jnp.where(col_z < MODES_Z // 2, col_z, col_z - MODES_Z)
    kx = wave_x * col_x.astype(jnp.float32)
    kz = wave_z * signed.astype(jnp.float32)
    return kx * kx + kz * kz + viscous_rate


def row_factors(w_ref, total, q, row, local, last, lam, lam2, s_next):
    at = lambda k: w_ref[(2 * k + q) * total + row]
    pivot = 1.0 + lam * at(1)
    if local < last:
        pivot = pivot - lam2 * at(3) * s_next
    s = 1.0 / pivot
    low = lam * at(0)
    if local == 0:
        low = low + jnp.where(row == 0, 1.0, 0.0)
    return s, low * s, lam * at(2)


def channel_kernel(n, nk, per, rows, tile, group, scale, w_hbm, f_hbm, x_buf, spec_ref,
                   w_ref, f_buf, e_buf, ls_buf, r_buf, sq_buf, both, y_send, y_recv, coef, elim, b_send, edge, mine, held,
                   table_sem, load_sem, dsend_sem, drecv_sem, ysend_sem, yrecv_sem, bsend_sem, erecv_sem, rsend_sem,
                   ssend_sem, srecv_sem):
    total = n * rows
    last = rows - 1
    me = lax.axis_index("gy")
    ka = lax.axis_index("ka")
    pairs = n * per * LANES
    count = group * per
    span = count * tile
    groups = n // group
    chips = n // 2
    chip, core = me // 2, lax.rem(me, 2)
    sibling = 2 * chip + 1 - core

    def nearest(k, here, size):
        return lax.bitwise_xor(here, k) if size & (size - 1) == 0 else lax.rem(here + k, size)

    def load(i):
        g = nearest(groups - 1 - i, me // group, groups)
        where = pl.ds(pl.multiple_of(g * span, span), span)
        return pltpu.make_async_copy(f_hbm.at[:, :, :, where, :], f_buf.at[:, :, :, where, :], load_sem.at[i])

    table = pltpu.make_async_copy(w_hbm, w_ref, table_sem)
    table.start()
    for i in range(groups):
        load(i).start()

    barrier = pltpu.get_barrier_semaphore()

    def greet(k, _):
        pl.semaphore_signal(barrier, inc=1, device_id={"gy": lax.rem(me + k, n)}, device_id_type=MESH)
        return 0

    lax.fori_loop(1, n, greet, 0)
    for k in range(1, nk):
        pl.semaphore_signal(barrier, inc=1, device_id={"ka": lax.rem(ka + k, nk)}, device_id_type=MESH)

    def d_copy(which, g):
        where = pl.ds(g * group, group)
        return pltpu.make_async_remote_copy(
            src_ref=both.at[which, where], dst_ref=both.at[which, where], send_sem=dsend_sem.at[g],
            recv_sem=drecv_sem.at[g], device_id={"gy": sibling}, device_id_type=MESH)

    def y_copy(to, frm):
        return pltpu.make_async_remote_copy(
            src_ref=y_send.at[to], dst_ref=y_recv.at[frm], send_sem=ysend_sem.at[to],
            recv_sem=yrecv_sem.at[frm], device_id={"gy": 2 * to + core}, device_id_type=MESH)

    def b_copy(to, owner):
        return pltpu.make_async_remote_copy(
            src_ref=b_send.at[to], dst_ref=edge.at[owner], send_sem=bsend_sem.at[to],
            recv_sem=erecv_sem.at[owner], device_id={"gy": 2 * to + core}, device_id_type=MESH)

    def r_copy(owner):
        return pltpu.make_async_remote_copy(
            src_ref=edge.at[owner], dst_ref=edge.at[owner], send_sem=rsend_sem.at[owner // 2],
            recv_sem=erecv_sem.at[owner], device_id={"gy": sibling}, device_id_type=MESH)

    def local_group(i):
        g = nearest(groups - 1 - i, me // group, groups)
        load(i).wait()
        part = pl.ds(pl.multiple_of(g * count, count), count)
        lam = shift_of(ka * pairs + g * (count * LANES), count)
        lam2 = lam * lam
        kappa = viscous_rate / lam
        for q in range(2):
            s = None
            e = [None, None]
            yl = [None, None]
            sums = [None, None]
            for j in range(last, -1, -1):
                row = me * rows + j
                s, ls, up = row_factors(w_ref, total, q, row, j, last, lam, lam2, s)
                right = s * up if j == last else (s * up) * right
                ls_buf[q, j, part] = ls
                r_buf[q, j, part] = right
                for p in range(2):
                    f = f_buf[p, q, j // tile, pl.ds(g * span + j % tile, count, stride=tile), :]
                    src = kappa * f
                    if j == last:
                        e[p] = s * src
                        yl[p] = e[p]
                        sums[p] = e[p] - src
                    else:
                        e[p] = s * (src + up * e[p])
                        yl[p] = yl[p] + carry * e[p]
                        sums[p] = sums[p] + (theta * e[p] - src)
                    e_buf[p, q, j, part] = e[p]
                if j == last:
                    end, beta = right, right
                    carry = ls
                    tau = ls
                else:
                    end = end + carry * right
                    beta = beta + theta * right
                    carry = carry * ls
                    tau = ls * theta
                theta = 1.0 + tau
            for k, value in enumerate((*e, *yl, *sums, ls, right, carry, end, tau, beta)):
                for m in range(group):
                    both[core, g * group + m, k, q] = value[m * per:(m + 1) * per]

        @pl.when(i == 0)
        def _():
            pl.semaphore_wait(barrier, n + nk - 2)

        d_copy(core, g).start()

    def combine_group(i):
        g = nearest(groups - 1 - i, me // group, groups)
        d_copy(1 - core, g).wait_recv()
        for m in range(group // 2):
            to = g * (group // 2) + m
            chunk = 2 * to + core
            low = [both[0, chunk, k] for k in range(12)]
            high = [both[1, chunk, k] for k in range(12)]
            inv = 1.0 / (1.0 - low[9] * high[6])
            for p in range(2):
                below = inv * (low[2 + p] + low[9] * high[p])
                above = high[p] + high[6] * below
                y_send[to, 0, p] = low[p] + low[7] * above
                y_send[to, 1, p] = high[2 + p] + high[8] * below
                y_send[to, 2, p] = (low[4 + p] + high[4 + p]) + (low[11] * above + high[10] * below)

            @pl.when(to != chip)
            def _():
                y_copy(to, chip).start()

    table.wait()

    def up_phase(i, _):
        @pl.when(i < groups)
        def _():
            local_group(i)

        @pl.when(i > 0)
        def _():
            combine_group(i - 1)

        return 0

    lax.fori_loop(0, groups + 1, up_phase, 0)
    y_recv[chip] = y_send[chip]

    lam = shift_of(ka * pairs + me * (per * LANES), per)
    lam2 = lam * lam
    unroll = 4 if n % 4 == 0 else 1

    def responses(i, _):
        for d in range(unroll):
            block = i * unroll + d
            for q in range(2):
                s = None
                for j in range(last, -1, -1):
                    row = block * rows + j
                    s, ls, up = row_factors(w_ref, total, q, row, j, last, lam, lam2, s)
                    if j == last:
                        e = s * up
                        yl = e
                        sums = e
                        carry = ls
                        tau = ls
                    else:
                        e = s * (up * e)
                        yl = yl + carry * e
                        sums = sums + (1.0 + tau) * e
                        carry = carry * ls
                        tau = ls * (1.0 + tau)
                for k, value in enumerate((ls, e, carry, yl, tau, sums)):
                    coef[block, k, q] = value
        return 0

    lax.fori_loop(0, n // unroll, responses, 0)

    def chip_responses(c, _):
        a0, b0, c0, d0, alpha0, beta0 = (coef[2 * c, k] for k in range(6))
        a1, b1, c1, d1, alpha1, beta1 = (coef[2 * c + 1, k] for k in range(6))
        inv = 1.0 / (1.0 - d0 * a1)
        low_left, low_right = inv * c0, inv * d0 * b1
        high_left, high_right = a1 * low_left, b1 * inv
        for k, value in enumerate((a0 + b0 * high_left, b0 * high_right, c1 * low_left, d1 + c1 * low_right,
                                   alpha0 + beta0 * high_left + alpha1 * low_left,
                                   beta1 + beta0 * high_right + alpha1 * low_right)):
            coef[c, k] = value
        return 0

    lax.fori_loop(0, chips, chip_responses, 0, unroll=chips <= 8)

    def y_arrived(k, _):
        y_copy(chip, lax.rem(chip + k, chips)).wait_recv()
        return 0

    lax.fori_loop(1, chips, y_arrived, 0)

    zero = jnp.zeros((2, per, LANES), jnp.float32)
    for k in range(3):
        elim[chips, k] = zero

    def up_sweep(k, state):
        g = chips - 1 - k
        f0, f1, phi, s0, s1, psi = state
        a, b, c, d, alpha, beta = (coef[g, m] for m in range(6))
        inv = 1.0 / (1.0 - d * phi)
        lamb = c * inv
        ls = [(y_recv[g, 1, p] + d * fp) * inv for p, fp in ((0, f0), (1, f1))]
        right = [fp + phi * l for fp, l in ((f0, ls[0]), (f1, ls[1]))]
        new_f = [y_recv[g, 0, p] + b * right[p] for p in range(2)]
        new_s = [y_recv[g, 2, p] + beta * right[p] + sp + psi * ls[p] for p, sp in ((0, s0), (1, s1))]
        new_phi = a + b * (phi * lamb)
        new_psi = alpha + beta * (phi * lamb) + psi * lamb
        elim[g, 0] = new_f[0]
        elim[g, 1] = new_f[1]
        elim[g, 2] = new_phi
        elim[g, 3] = ls[0]
        elim[g, 4] = ls[1]
        elim[g, 5] = lamb
        return new_f[0], new_f[1], new_phi, new_s[0], new_s[1], new_psi

    state = lax.fori_loop(0, chips, up_sweep, (zero,) * 6, unroll=chips <= 8)
    wall = 1.0 / state[5]

    def down_sweep(g, left):
        b_send[g, 0, 0] = left[0]
        b_send[g, 0, 1] = left[1]
        new = [elim[g, 3 + p] + elim[g, 5] * left[p] for p in range(2)]
        for p in range(2):
            b_send[g, 1, p] = elim[g + 1, p] + elim[g + 1, 2] * new[p]

        @pl.when(g != chip)
        def _():
            b_copy(g, me).start()

        return new[0], new[1]

    lax.fori_loop(0, chips, down_sweep, (-state[3] * wall, -state[4] * wall), unroll=chips <= 8)
    edge[me] = b_send[chip]
    sq_buf[...] = jnp.zeros_like(sq_buf)

    def relay_group(i):
        g = nearest(i, me // group, groups)
        for m in range(group // 2):
            owner = g * group + 2 * m + core

            @pl.when(owner != me)
            def _():
                b_copy(chip, owner).wait_recv()

            r_copy(owner).start()

    def close_group(i):
        g = nearest(i, me // group, groups)
        for m in range(group // 2):
            r_copy(g * group + 2 * m + 1 - core).wait_recv()
        part = pl.ds(pl.multiple_of(g * count, count), count)
        lam = shift_of(ka * pairs + g * (count * LANES), count)
        kappa = viscous_rate / lam
        joined = lambda get: jnp.concatenate([get(g * group + m) for m in range(group)], axis=0)
        for q in range(2):
            low = [joined(lambda c: both[0, c, k, q]) for k in range(12)]
            high = [joined(lambda c: both[1, c, k, q]) for k in range(12)]
            inv = 1.0 / (1.0 - low[9] * high[6])
            z, after = [], []
            for p in range(2):
                outer_left = joined(lambda c: edge[c, 0, p, q])
                outer_right = joined(lambda c: edge[c, 1, p, q])
                below = inv * (low[2 + p] + low[9] * (high[p] + high[7] * outer_right) + low[8] * outer_left)
                above = high[p] + high[6] * below + high[7] * outer_right
                z.append(jnp.where(core == 0, outer_left, below))
                after.append(jnp.where(core == 0, above, outer_right))
            for j in range(rows):
                ls = ls_buf[q, j, part]
                right = r_buf[q, j, part]
                square = None
                for p in range(2):
                    where = (p, q, j // tile, pl.ds(g * span + j % tile, count, stride=tile), slice(None))
                    z[p] = (e_buf[p, q, j, part] + right * after[p]) + ls * z[p]
                    x = z[p] - kappa * f_buf[where]
                    x_buf[where] = x
                    square = x * x if p == 0 else square + x * x
                sq_buf[q, j] += sum(square[m * per:(m + 1) * per] for m in range(group))

    def down_phase(i, _):
        @pl.when(i < groups)
        def _():
            relay_group(i)

        @pl.when(i > 0)
        def _():
            close_group(i - 1)

        return 0

    lax.fori_loop(0, groups + 1, down_phase, 0)

    mine[...] = jnp.sum(sq_buf[...], axis=2)

    def s_copy(k):
        return pltpu.make_async_remote_copy(
            src_ref=mine, dst_ref=held.at[k - 1], send_sem=ssend_sem.at[k - 1], recv_sem=srecv_sem.at[k - 1],
            device_id={"ka": lax.rem(ka + k, nk)}, device_id_type=MESH)

    for k in range(1, nk):
        s_copy(k).start()

    def sent(k, _):
        to = lax.rem(chip + k, chips)
        y_copy(to, chip).wait_send()
        b_copy(to, me).wait_send()
        return 0

    lax.fori_loop(1, chips, sent, 0)

    def relayed(c, _):
        r_copy(2 * c + core).wait_send()
        return 0

    lax.fori_loop(0, chips, relayed, 0)

    def given(g, _):
        d_copy(core, g).wait_send()
        return 0

    lax.fori_loop(0, groups, given, 0)
    added = mine[...]
    for k in range(1, nk):
        s_copy(k).wait_recv()
        added = added + held[k - 1]
    ones = jnp.ones((8, LANES), jnp.float32)
    for q in range(2):
        sums = lax.dot_general(ones, added[q], (((1,), (1,)), ((), ())), precision=lax.Precision.HIGHEST,
                               preferred_element_type=jnp.float32)
        spec_ref[q:q + 1, :] = sums[0:1] * scale
    for k in range(1, nk):
        s_copy(k).wait_send()


def per_device(n, nk, driving_coefficients):
    _, pairs, _, rows = driving_coefficients.shape
    per = pairs // (LANES * n)
    tile = 8 if rows % 8 == 0 else 1
    cols = pairs // LANES
    chips = n // 2
    group = next((g for g in range(2, n) if n % g == 0 and g * per * tile % 8 == 0), n)
    span = group * per * tile
    f = jnp.transpose(driving_coefficients, (0, 2, 3, 1)).reshape(2, 2, rows // tile, tile, cols, LANES)
    f = jnp.swapaxes(f, 3, 4).reshape(2, 2, rows // tile, cols * tile, LANES)
    table = jnp.asarray(weight_table(n * rows))
    vmem = pl.BlockSpec(memory_space=pltpu.VMEM)
    f32 = jnp.float32
    x, spectrum = pl.pallas_call(
        functools.partial(channel_kernel, n, nk, per, rows, tile, group, 1.0 / (2.0 * pairs * nk)),
        out_shape=(jax.ShapeDtypeStruct(f.shape, f32), jax.ShapeDtypeStruct((2, rows), f32)),
        in_specs=[pl.BlockSpec(memory_space=pltpu.HBM)] * 2,
        out_specs=(vmem, vmem),
        scratch_shapes=[
            pltpu.SMEM(table.shape, f32),
            pltpu.VMEM(f.shape, f32),
            pltpu.VMEM((2, 2, rows, cols, LANES), f32),
            pltpu.VMEM((2, rows, cols, LANES), f32),
            pltpu.VMEM((2, rows, cols, LANES), f32),
            pltpu.VMEM((2, rows, per, LANES), f32),
            pltpu.VMEM((2, n, 12, 2, per, LANES), f32),
            pltpu.VMEM((chips, 3, 2, 2, per, LANES), f32),
            pltpu.VMEM((chips, 3, 2, 2, per, LANES), f32),
            pltpu.VMEM((n, 6, 2, per, LANES), f32),
            pltpu.VMEM((chips + 1, 6, 2, per, LANES), f32),
            pltpu.VMEM((chips, 2, 2, 2, per, LANES), f32),
            pltpu.VMEM((n, 2, 2, 2, per, LANES), f32),
            pltpu.VMEM((2, rows, LANES), f32),
            pltpu.VMEM((nk - 1, 2, rows, LANES), f32),
            pltpu.SemaphoreType.DMA,
            *[pltpu.SemaphoreType.DMA((n // group,))] * 3,
            *[pltpu.SemaphoreType.DMA((chips,))] * 3,
            pltpu.SemaphoreType.DMA((n,)),
            pltpu.SemaphoreType.DMA((chips,)),
            pltpu.SemaphoreType.DMA((nk - 1,)),
            pltpu.SemaphoreType.DMA((nk - 1,)),
        ],
        compiler_params=pltpu.CompilerParams(collective_id=0, has_side_effects=True, vmem_limit_bytes=24 << 20),
        name="channel_substep",
    )(*(pltpu.with_memory_space_constraint(given, pltpu.HBM) for given in (table, f)))
    x = jnp.swapaxes(x.reshape(2, 2, rows // tile, cols, tile, LANES), 3, 4).reshape(2, 2, rows, pairs)
    return jnp.transpose(x, (0, 3, 1, 2)), spectrum


def solution(mesh):
    n, nk = mesh.shape["gy"], mesh.shape["ka"]
    return jax.shard_map(
        functools.partial(per_device, n, nk), mesh=mesh,
        in_specs=(P(None, "ka", None, "gy"),),
        out_specs=(P(None, "ka", None, "gy"), P(None, "gy")), check_vma=False,
    )
```
